32 devices in a mesh: dev: 32 (over z, y, x, core).
Axes of the slice: x: 2, y: 2, z: 4, core: 2. Of those that a mesh axis runs over, the one named last changes fastest.
Arguments:
- dual_blocks: bfloat16 [32, 3072, 3072], P('dev'), as said below
- rigid_modes: float32 [32, 6, 3072], P('dev'), may hold values from -5 to 5
- dual_local: float32 [32, 8, 3072], P('dev'), may hold values from -6 to 6
- coarse_rhs: float32 [32, 6, 8], P('dev'), may hold values from -4608 to 4608
- iface_sizes: int32 [32], P('dev'), may hold values from 1536 to 3072, as said below
- neighbours: int32 [32, 6], P('dev'), may hold values from -1 to 31, as said below
- shared_counts: int32 [32, 6], P('dev'), may hold values from 256 to 512, as said below
- iface_map: int32 [32, 3072], P('dev'), may hold values from -1 to 3071, as said below
- owner: int32 [32], replicated, may hold values from 0 to 31, as said below
Outputs:
- multipliers: float32 [32, 8, 3072], P('dev')
- projected_residual: float32 [32, 8, 3072], P('dev')
The draws below stay inside these ranges and needn't reach their ends.
Inputs may be any that keep to these rules, and one draw needn't show every extreme that they name: `dual_blocks`: each block is symmetric positive definite, and so is each of its leading principal parts. Grid subdomain g is held by slot owner[g] = (g + s) mod 32 for one offset s of the draw, so the subdomains across the faces -x, +x, -y, +y, -z, +z of slot i sit in slots i - 1, i + 1, i - 4, i + 4, i - 16, i + 16, taken mod 32. `neighbours`: the subdomains form a grid of 4 x 4 x 32/16 with g = x + 4 y + 16 z. Row i lists, for the faces -x, +x, -y, +y, -z, +z of the subdomain held in slot i, the grid subdomain across that face, or -1 on the outer boundary; across a face from g the opposite face names g. `shared_counts`: equal on both sides of a shared face; some subdomain has 512 on all its faces. `iface_sizes`: the sum of the slot's shared_counts row; some subdomain has 3072. `iface_map`: for j < iface_sizes[i], entry j is f * 512 + p for the dof at position p of face f of slot i (p below that face's count), each such code once; -1 beyond. The dof at position p of a shared face pairs with the dof at position p of the opposite face of the neighbour.
All inputs are finite; a program needn't handle non-finite values.
Results may differ from the reference program's by a relative error of at most 0.025.
Values sent between devices are 32-bit elements; how exact they have to be, the bound alone decides.
A program may use at most 128 MiB of HBM per device.

```python
import math
import jax
import jax.numpy as jnp
from jax import lax

FACES = 6
MODES = 6
CAP = 512
NMAX = 3072
LOADS = 8
ITERS = 3
NSUB = 32


def grid_links():
    layers = NSUB // 16
    identity = jnp.arange(NSUB, dtype=jnp.int32)
    along_x = identity % 4
    along_y = identity // 4 % 4
    along_z = identity // 16
    columns = [jnp.where(along_x > 0, identity - 1, -1), jnp.where(along_x < 3, identity + 1, -1), jnp.where(along_y > 0, identity - 4, -1), jnp.where(along_y < 3, identity + 4, -1), jnp.where(along_z > 0, identity - 16, -1), jnp.where(along_z < layers - 1, identity + 16, -1)]
    return jnp.stack(columns, axis=1).astype(jnp.int32)


def layout_draw(key):
    base = jax.random.fold_in(key, 7301)
    key_count, key_star, key_owner, key_order = jax.random.split(base, 4)
    links = grid_links()
    drawn = jax.random.randint(key_count, (NSUB, FACES), CAP // 2, CAP + 1, dtype=jnp.int32)
    star = jax.random.randint(key_star, (), 0, NSUB, dtype=jnp.int32)
    drawn = drawn.at[star].set(CAP)
    for lower_face in (0, 2, 4):
        across = links[star, lower_face]
        drawn = drawn.at[jnp.where(across < 0, star, across), lower_face + 1].set(CAP)
    counts = drawn
    for lower_face in (0, 2, 4):
        across = links[:, lower_face]
        mirrored = drawn[jnp.clip(across, 0, NSUB - 1), lower_face + 1]
        counts = counts.at[:, lower_face].set(jnp.where(across < 0, drawn[:, lower_face], mirrored))
    offset = jax.random.randint(key_owner, (), 1, NSUB, dtype=jnp.int32)
    identity = jnp.arange(NSUB, dtype=jnp.int32)
    owner = ((identity + offset) % NSUB).astype(jnp.int32)
    hosted = ((identity - offset + NSUB) % NSUB).astype(jnp.int32)
    slot_links = links[hosted]
    slot_counts = counts[hosted]
    sizes = jnp.sum(slot_counts, axis=1).astype(jnp.int32)
    codes_all = jnp.arange(FACES * CAP, dtype=jnp.int32)
    live_codes = (codes_all % CAP)[None, :] < slot_counts[:, codes_all // CAP]
    slot_keys = jax.random.split(key_order, NSUB)
    shuffles = jax.vmap(lambda slot_key: jax.random.permutation(slot_key, FACES * CAP))(slot_keys).astype(jnp.int32)
    scores = shuffles + jnp.where(live_codes, 0, FACES * CAP).astype(jnp.int32)
    ordered = jnp.argsort(scores, axis=1, stable=True).astype(jnp.int32)
    positions = jnp.arange(NMAX, dtype=jnp.int32)
    iface_map = jnp.where(positions[None, :] < sizes[:, None], ordered, -1).astype(jnp.int32)
    return (owner, sizes, slot_links, slot_counts, iface_map, hosted)


def draw_owner(key, part):
    return layout_draw(key)[0]


def draw_iface_sizes(key, part):
    return layout_draw(key)[1]


def draw_neighbours(key, part):
    return layout_draw(key)[2]


def draw_shared_counts(key, part):
    return layout_draw(key)[3]


def draw_iface_map(key, part):
    return layout_draw(key)[4]


def mode_sample(sample_key, shape):
    values = jnp.clip(jax.random.normal(sample_key, shape, jnp.float32), -4.0, 4.0)
    return values


def draw_rigid_modes(key, part):
    owner, sizes, slot_links, slot_counts, iface_map, hosted = layout_draw(key)
    base = jax.random.fold_in(key, 7303)
    key_common, key_edge, key_own = jax.random.split(base, 3)
    common = mode_sample(key_common, (NSUB, 3, MODES, CAP))
    edge = mode_sample(key_edge, (NSUB, FACES, MODES, CAP))
    own = mode_sample(key_own, (NSUB, MODES, NMAX))
    face_ids = jnp.arange(FACES, dtype=jnp.int32)
    upper = face_ids % 2 == 1
    face_key = jnp.where(upper[None, :], hosted[:, None], slot_links)
    face_key = jnp.clip(face_key, 0, NSUB - 1).astype(jnp.int32)
    axis_ids = (face_ids // 2).astype(jnp.int32)
    face_vals = common[face_key, axis_ids[None, :]]
    face_vals = jnp.where((slot_links >= 0)[:, :, None, None], face_vals, edge)
    flattened = jnp.transpose(face_vals, (0, 2, 1, 3)).reshape(NSUB, MODES, FACES * CAP)
    codes = jnp.clip(iface_map, 0, FACES * CAP - 1).astype(jnp.int32)
    gather_index = jnp.broadcast_to(codes[:, None, :], (NSUB, MODES, NMAX))
    picked = jnp.take_along_axis(flattened, gather_index, axis=2)
    return (picked + 0.25 * own).astype(jnp.float32)


def draw_dual_blocks(key, part):
    slot_keys = jax.random.split(jax.random.fold_in(key, 7302), NSUB)
    spread = 0.3 / math.sqrt(NMAX)

    def single(slot_key):
        key_off, key_diag = jax.random.split(slot_key)
        entries = jax.random.normal(key_off, (NMAX, NMAX), jnp.float32)
        symmetric = (entries + entries.T) * (spread / math.sqrt(2.0))
        diag_vals = jax.random.uniform(key_diag, (NMAX,), jnp.float32, 1.0, 1.5)
        return (symmetric + jnp.diag(diag_vals)).astype(jnp.bfloat16)
    return jax.lax.map(single, slot_keys)


def block_levels(stream_key, shape, shards, smallest, largest):
    loudness, own = 1.0, jax.random.fold_in(stream_key, 6)
    for dim, shards_of in shards:
        steps = jnp.exp(jax.random.uniform(jax.random.fold_in(own, dim), (shards_of,), jnp.float32, smallest / len(shards), largest / len(shards)))
        loudness = loudness * jnp.repeat(steps, shape[dim] // shards_of).reshape([-1 if axis == dim else 1 for axis in range(len(shape))])
    return loudness


def normal_values(stream_key, extent, scale, bound, cuts=(), kind=jnp.bfloat16):
    values = scale * jax.random.normal(stream_key, extent, jnp.float32)
    if cuts:
        values = values * block_levels(stream_key, extent, cuts, -0.22, 0.18)
    return jnp.clip(values, -bound, bound).astype(kind)


def setup_inputs(seed: int = 0) -> dict:
    key_list = jax.random.split(jax.random.key(seed), 10)
    dual_blocks = draw_dual_blocks(jax.random.fold_in(key_list[9], 71), 0)
    rigid_modes = draw_rigid_modes(jax.random.fold_in(key_list[9], 71), 0)
    dual_local = normal_values(key_list[2], (NSUB, LOADS, NMAX), 1.0, 6.0, ((0, 32),), jnp.float32)
    coarse_rhs = normal_values(key_list[3], (NSUB, MODES, LOADS), (NMAX // 4), 4608.0, ((0, 32),), jnp.float32)
    iface_sizes = draw_iface_sizes(jax.random.fold_in(key_list[9], 71), 0)
    neighbours = draw_neighbours(jax.random.fold_in(key_list[9], 71), 0)
    shared_counts = draw_shared_counts(jax.random.fold_in(key_list[9], 71), 0)
    iface_map = draw_iface_map(jax.random.fold_in(key_list[9], 71), 0)
    owner = draw_owner(jax.random.fold_in(key_list[9], 71), 0)
    return {"dual_blocks": dual_blocks, "rigid_modes": rigid_modes, "dual_local": dual_local, "coarse_rhs": coarse_rhs, "iface_sizes": iface_sizes, "neighbours": neighbours, "shared_counts": shared_counts, "iface_map": iface_map, "owner": owner}


OPPOSITE = (1, 0, 3, 2, 5, 4)
HIGHEST_PRECISION = lax.Precision.HIGHEST

def tables(iface_sizes, neighbours, shared_counts, iface_map, owner):
    columns = jnp.arange(NMAX, dtype=jnp.int32)
    live_dofs = columns[None, :] < iface_sizes[:, None]
    dof_codes = jnp.clip(jnp.where(live_dofs, iface_map, 0), 0, FACES * CAP - 1).astype(jnp.int32)
    which_face = dof_codes // CAP
    position = dof_codes % CAP
    face_owner = jnp.take_along_axis(neighbours, which_face, axis=1)
    face_count = jnp.take_along_axis(shared_counts, which_face, axis=1)
    shared = live_dofs & (face_owner >= 0) & (position < face_count)
    weights = jnp.where(shared, 0.5, jnp.where(live_dofs, 1.0, 0.0)).astype(jnp.float32)
    row_index = jnp.broadcast_to(jnp.arange(NSUB, dtype=jnp.int32)[:, None], (NSUB, NMAX))
    targets = jnp.where(live_dofs, dof_codes, FACES * CAP).astype(jnp.int32)
    inverse = jnp.full((NSUB, FACES * CAP), NMAX, jnp.int32)
    inverse = inverse.at[row_index, targets].set(jnp.broadcast_to(columns[None, :], (NSUB, NMAX)), mode='drop')
    partner_slot = jnp.where(neighbours >= 0, owner[jnp.clip(neighbours, 0, NSUB - 1)], 0).astype(jnp.int32)
    face_mask = ((neighbours >= 0)[:, :, None] & (jnp.arange(CAP, dtype=jnp.int32)[None, None, :] < shared_counts[:, :, None])).astype(jnp.float32)
    return (live_dofs, dof_codes, shared, weights, inverse, partner_slot, face_mask)

def to_faces(values, inverse):
    padded = jnp.concatenate([values, jnp.zeros((values.shape[0], values.shape[1], 1), values.dtype)], axis=2)
    gather_index = jnp.broadcast_to(inverse[:, None, :], (values.shape[0], values.shape[1], FACES * CAP))
    return jnp.take_along_axis(padded, gather_index, axis=2).reshape(values.shape[0], values.shape[1], FACES, CAP)

def partner_faces(face_vals, partner_slot, face_mask):
    opposite = jnp.array(OPPOSITE, jnp.int32)
    swapped = jnp.transpose(face_vals, (0, 2, 1, 3))
    picked = swapped[partner_slot, opposite[None, :]]
    return picked * face_mask[:, :, None, :]

def to_dofs(far_faces, dof_codes, shared):
    flattened = jnp.transpose(far_faces, (0, 2, 1, 3)).reshape(far_faces.shape[0], far_faces.shape[2], FACES * CAP)
    gather_index = jnp.broadcast_to(dof_codes[:, None, :], (far_faces.shape[0], far_faces.shape[2], NMAX))
    return jnp.take_along_axis(flattened, gather_index, axis=2) * shared.astype(jnp.float32)[:, None, :]

def assemble(values, layout):
    live_dofs, dof_codes, shared, weights, inverse, partner_slot, face_mask = layout
    far_faces = partner_faces(to_faces(values, inverse), partner_slot, face_mask)
    return live_dofs.astype(jnp.float32)[:, None, :] * (values - to_dofs(far_faces, dof_codes, shared))

def dual_products(dual_blocks, vectors):

    def single(operands):
        dual_block, vector = operands
        return lax.dot_general(vector.astype(jnp.bfloat16).astype(jnp.float32), dual_block.astype(jnp.float32), (((1,), (1,)), ((), ())), preferred_element_type=jnp.float32)
    return lax.map(single, (dual_blocks, vectors))

def solve_coarse(factor, vector):
    middle = lax.linalg.triangular_solve(factor, vector, left_side=True, lower=True)
    return lax.linalg.triangular_solve(factor, middle, left_side=True, lower=True, transpose_a=True)

def weighted_inner(weights, left_vec, right_vec):
    return jnp.sum(weights[:, None, :] * left_vec * right_vec, axis=(0, 2))

def reference(dual_blocks, rigid_modes, dual_local, coarse_rhs, iface_sizes, neighbours, shared_counts, iface_map, owner):
    layout = tables(iface_sizes, neighbours, shared_counts, iface_map, owner)
    live_dofs, dof_codes, shared, weights, inverse, partner_slot, face_mask = layout
    live_float = live_dofs.astype(jnp.float32)
    modes_live = rigid_modes * live_float[:, None, :]
    own_modes = to_faces(modes_live, inverse)
    far_modes = partner_faces(own_modes, partner_slot, face_mask)
    diagonal = jnp.einsum('iaj,ibj->iab', modes_live, modes_live, precision=HIGHEST_PRECISION)
    coupling = -jnp.einsum('iafp,ifbp->ifab', own_modes, far_modes, precision=HIGHEST_PRECISION)
    slot_index = jnp.arange(NSUB, dtype=jnp.int32)
    coarse_blocks = jnp.zeros((NSUB, MODES, NSUB, MODES), jnp.float32)
    coarse_blocks = coarse_blocks.at[slot_index, :, slot_index, :].set(diagonal)
    coarse_blocks = coarse_blocks.at[slot_index[:, None], :, partner_slot, :].add(coupling)
    factor = jnp.linalg.cholesky(coarse_blocks.reshape(NSUB * MODES, NSUB * MODES))

    def modes_apply(solution):
        stacked = solution.reshape(NSUB, MODES, LOADS)
        own_part = jnp.einsum('iaj,ial->ilj', modes_live, stacked, precision=HIGHEST_PRECISION)
        return assemble(own_part, layout)

    def project(residual):
        coarse_all = jnp.einsum('iaj,ilj->ial', modes_live, residual, precision=HIGHEST_PRECISION).reshape(NSUB * MODES, LOADS)
        projected = residual - modes_apply(solve_coarse(factor, coarse_all))
        return (projected, weighted_inner(weights, projected, projected))

    def dual_apply(vector):
        return assemble(dual_products(dual_blocks, vector), layout)
    dual_rhs = assemble(dual_local, layout)
    multipliers = modes_apply(solve_coarse(factor, coarse_rhs.reshape(NSUB * MODES, LOADS)))
    residual = dual_rhs - dual_apply(multipliers)
    projected, norm_sq = project(residual)
    direction = projected
    for step_index in range(ITERS):
        applied = dual_apply(direction)
        step_size = norm_sq / weighted_inner(weights, direction, applied)
        multipliers = multipliers + step_size[None, :, None] * direction
        residual = residual - step_size[None, :, None] * applied
        projected, norm_next = project(residual)
        direction = projected + (norm_next / norm_sq)[None, :, None] * direction
        norm_sq = norm_next
    return (multipliers, projected)
```

```python
import functools

import jax
import jax.numpy as jnp
from jax import lax
from jax.experimental import pallas as pl
from jax.experimental.pallas import tpu as pltpu
from jax.sharding import PartitionSpec as P

FACES = 6
MODES = 6
ITERS = 3
LANES = 128
ROWS = 256
FACE_STEPS = (-1, 1, -4, 4, -16, 16)
HIGHEST = lax.Precision.HIGHEST


def params(steps=None):
    if steps is None:
        return pltpu.CompilerParams(vmem_limit_bytes=50 * 2**20)
    return pltpu.CompilerParams(
        dimension_semantics=("arbitrary",), vmem_limit_bytes=50 * 2**20
    )


def gather_lanes(source, index_ref, block):
    index = jnp.broadcast_to(index_ref[pl.ds(block, 1), :], (source.shape[0], LANES))
    low = jnp.bitwise_and(index, LANES - 1)
    high = jnp.right_shift(index, 7)
    picked = jnp.zeros((source.shape[0], LANES), jnp.float32)
    for part in range(source.shape[1] // LANES):
        taken = jnp.take_along_axis(
            source[:, part * LANES : (part + 1) * LANES], low, axis=1, mode="promise_in_bounds"
        )
        picked = jnp.where(high == part, taken, picked)
    return picked


def setup_kernel(codes_ref, values_ref, modes_ref, rhs_ref, inverse_ref, onehot_ref, left_ref):
    codes = codes_ref[...]
    nmax = codes.shape[1]
    blocks = nmax // LANES
    wide = left_ref.shape[0] // 3
    columns = lax.broadcasted_iota(jnp.int32, (1, nmax), 1)
    high = jnp.right_shift(codes, 7)
    low = jnp.where(codes < 0, -1, jnp.bitwise_and(codes, LANES - 1))
    rows = lax.broadcasted_iota(jnp.int32, (LANES, nmax), 0)
    onehot_ref[...] = jnp.where(rows == low, 1.0, 0.0).astype(jnp.bfloat16)
    hit = lax.broadcasted_iota(jnp.int32, (wide, nmax), 0) == high
    upper = jnp.right_shift(columns, 7).astype(jnp.float32)
    lower = jnp.bitwise_and(columns, LANES - 1).astype(jnp.float32)
    left_ref[:wide, :] = jnp.where(hit, upper, 0.0).astype(jnp.bfloat16)
    left_ref[wide : 2 * wide, :] = jnp.where(hit, lower, 0.0).astype(jnp.bfloat16)
    left_ref[2 * wide :, :] = jnp.where(hit, 1.0, 0.0).astype(jnp.bfloat16)
    found = lax.dot_general(
        left_ref[...], onehot_ref[...], (((1,), (1,)), ((), ())),
        preferred_element_type=jnp.float32,
    )
    place = found[:wide] * LANES + found[wide : 2 * wide]
    place = jnp.where(found[2 * wide :] > 0.5, place, float(nmax))
    inverse_ref[...] = (place[:blocks] + 0.5).astype(jnp.int32)

    def body(block, carry):
        start = pl.multiple_of(block * LANES, LANES)
        modes_ref[:, pl.ds(start, LANES)] = gather_lanes(values_ref.at[0], inverse_ref, block)
        rhs_ref[:, pl.ds(start, LANES)] = gather_lanes(values_ref.at[1], inverse_ref, block)
        return carry

    lax.fori_loop(0, blocks, body, 0)


def invert_kernel(matrix_ref, out_ref):
    size, width = out_ref.shape
    out_ref[...] = matrix_ref[...]
    lane = lax.broadcasted_iota(jnp.int32, (1, width), 1)

    def body(step, carry):
        k = 2 * step
        at0, at1 = lane == k, lane == k + 1
        row0 = out_ref[pl.ds(k, 1), :]
        row1 = out_ref[pl.ds(k + 1, 1), :]
        p00 = jnp.sum(jnp.where(at0, row0, 0.0), axis=1, keepdims=True)
        p01 = jnp.sum(jnp.where(at1, row0, 0.0), axis=1, keepdims=True)
        p11 = jnp.sum(jnp.where(at1, row1, 0.0), axis=1, keepdims=True)
        first = 1.0 / p00
        ratio = p01 * first
        i11 = 1.0 / (p11 - p01 * ratio)
        i01 = -ratio * i11
        i00 = first + ratio * ratio * i11
        use0 = i00 * row0 + i01 * row1
        use1 = i01 * row0 + i11 * row1
        whole = out_ref[...]
        col0 = jnp.sum(jnp.where(at0, whole, 0.0), axis=1, keepdims=True)
        col1 = jnp.sum(jnp.where(at1, whole, 0.0), axis=1, keepdims=True)
        fresh = whole - col0 * use0 - col1 * use1
        fresh = jnp.where(at0, col0 * i00 + col1 * i01, fresh)
        fresh = jnp.where(at1, col0 * i01 + col1 * i11, fresh)
        out_ref[...] = fresh
        out_ref[pl.ds(k, 1), :] = jnp.where(at0, -i00, jnp.where(at1, -i01, use0))
        out_ref[pl.ds(k + 1, 1), :] = jnp.where(at0, -i01, jnp.where(at1, -i11, use1))
        return carry

    lax.fori_loop(0, size // 2, body, 0)
    out_ref[...] = -out_ref[...]


def coarse_apply(coarse, picks_ref, modes_ref, far_ref, cap):
    z = lax.dot_general(
        coarse, picks_ref[...], (((1,), (0,)), ((), ())),
        precision=HIGHEST, preferred_element_type=jnp.float32,
    )
    blocks = []
    for face in range(FACES):
        span = slice(face * cap, (face + 1) * cap)
        total = jnp.zeros((coarse.shape[0], cap), jnp.float32)
        for mode in range(MODES):
            total += z[:, mode : mode + 1] * modes_ref[mode : mode + 1, span]
            column = (face + 1) * MODES + mode
            total -= z[:, column : column + 1] * far_ref[mode : mode + 1, span]
        blocks.append(total)
    return blocks


def product_steps(step, steps, vector_ref, map_ref, inverse_ref, dual_ref, sum_ref, outs, cap):
    per_step = dual_ref.shape[1] // LANES
    pieces = [gather_lanes(vector_ref, map_ref, step * per_step + i) for i in range(per_step)]
    vector = jnp.concatenate(pieces, axis=1).astype(jnp.bfloat16)
    part = jnp.dot(vector, dual_ref[0], preferred_element_type=jnp.float32)

    @pl.when(step == 0)
    def _():
        sum_ref[...] = part

    @pl.when(step > 0)
    def _():
        sum_ref[...] += part

    @pl.when(step == steps - 1)
    def _():
        def body(block, carry):
            start = pl.multiple_of(block * LANES, LANES)
            for face in range(FACES):
                outs[face][:, pl.ds(start, LANES)] = gather_lanes(
                    sum_ref, inverse_ref, face * (cap // LANES) + block
                )
            return carry

        lax.fori_loop(0, cap // LANES, body, 0)


def start_kernel(
    steps, cap, coarse_ref, picks_ref, modes_ref, far_ref, map_ref, inverse_ref, dual_ref,
    mult_ref, *rest,
):
    outs, sum_ref = rest[:FACES], rest[FACES]
    step = pl.program_id(0)

    @pl.when(step == 0)
    def _():
        parts = coarse_apply(coarse_ref[...], picks_ref, modes_ref, far_ref, cap)
        for face, part in enumerate(parts):
            mult_ref[:, face * cap : (face + 1) * cap] = part

    product_steps(step, steps, mult_ref, map_ref, inverse_ref, dual_ref, sum_ref, outs, cap)


def first_kernel(
    steps, cap, gathered_ref, picks_ref, modes_ref, far_ref, residual_ref, map_ref, inverse_ref,
    dual_ref, w_ref, *rest,
):
    outs, sum_ref = rest[:FACES], rest[FACES]
    step = pl.program_id(0)

    @pl.when(step == 0)
    def _():
        coarse = jnp.sum(gathered_ref[...], axis=0)
        parts = coarse_apply(coarse, picks_ref, modes_ref, far_ref, cap)
        for face, part in enumerate(parts):
            span = slice(face * cap, (face + 1) * cap)
            w_ref[:, span] = residual_ref[:, span] - part

    product_steps(step, steps, w_ref, map_ref, inverse_ref, dual_ref, sum_ref, outs, cap)


def advance(
    cap, slots, gathered_ref, picks_ref, modes_ref, far_ref, state, applied_ref, scalars_ref, outs
):
    mult_ref, w_ref, d_ref, q_ref, s_ref = state
    mult_out, w_out, d_out, q_out, s_out, scalars_out = outs
    coarse = jnp.sum(gathered_ref[...], axis=0)
    base = slots * MODES
    rho, wa, wq, da = (coarse[:, base + i : base + i + 1] for i in range(4))
    rho_old, dq_old = scalars_ref[:, 0:1], scalars_ref[:, 1:2]
    beta = rho / rho_old
    dq = wa + beta * (wq + da) + beta * beta * dq_old
    alpha = rho / dq
    parts = coarse_apply(coarse, picks_ref, modes_ref, far_ref, cap)
    for face, part in enumerate(parts):
        span = slice(face * cap, (face + 1) * cap)
        applied = applied_ref[:, span]
        d = w_ref[:, span] + beta * d_ref[:, span]
        s = applied - part + beta * s_ref[:, span]
        mult_out[:, span] = mult_ref[:, span] + alpha * d
        w_out[:, span] = w_ref[:, span] - alpha * s
        if d_out is not None:
            d_out[:, span] = d
            s_out[:, span] = s
            q_out[:, span] = applied + beta * q_ref[:, span]
    if scalars_out is not None:
        lane = lax.broadcasted_iota(jnp.int32, scalars_out.shape, 1)
        scalars_out[...] = jnp.where(lane == 0, rho, jnp.where(lane == 1, dq, 0.0))


def step_kernel(
    steps, cap, slots, gathered_ref, picks_ref, modes_ref, far_ref, m_ref, w_ref, d_ref, q_ref,
    s_ref, applied_ref, scalars_ref, map_ref, inverse_ref, dual_ref,
    m_out, w_out, d_out, q_out, s_out, scalars_out, *rest,
):
    outs, sum_ref = rest[:FACES], rest[FACES]
    step = pl.program_id(0)

    @pl.when(step == 0)
    def _():
        advance(
            cap, slots, gathered_ref, picks_ref, modes_ref, far_ref,
            (m_ref, w_ref, d_ref, q_ref, s_ref), applied_ref, scalars_ref,
            (m_out, w_out, d_out, q_out, s_out, scalars_out),
        )

    product_steps(step, steps, w_out, map_ref, inverse_ref, dual_ref, sum_ref, outs, cap)


def last_kernel(
    cap, slots, gathered_ref, picks_ref, modes_ref, far_ref, m_ref, w_ref, d_ref, q_ref, s_ref,
    applied_ref, scalars_ref, map_ref, m_out, w_out, m_tmp, w_tmp,
):
    advance(
        cap, slots, gathered_ref, picks_ref, modes_ref, far_ref,
        (m_ref, w_ref, d_ref, q_ref, s_ref), applied_ref, scalars_ref,
        (m_tmp, w_tmp, None, None, None, None),
    )

    def body(block, carry):
        start = pl.multiple_of(block * LANES, LANES)
        m_out[0, :, pl.ds(start, LANES)] = gather_lanes(m_tmp, map_ref, block)
        w_out[0, :, pl.ds(start, LANES)] = gather_lanes(w_tmp, map_ref, block)
        return carry

    lax.fori_loop(0, m_tmp.shape[1] // LANES, body, 0)


def combine_kernel(cap, slots, initial, slot_ref, modes_ref, masks_ref, *rest):
    own, far, rest = rest[:FACES], rest[FACES : 2 * FACES], rest[2 * FACES :]
    if initial:
        rhs_ref, rhs_far_ref, out_ref, sums_ref = rest
    else:
        w_ref, d_ref, q_ref, out_ref, sums_ref = rest
    loads = own[0].shape[0]
    counts = MODES if initial else MODES + 4
    totals = [jnp.zeros((loads, cap), jnp.float32) for _ in range(counts)]
    for face in range(FACES):
        span = slice(face * cap, (face + 1) * cap)
        shared = masks_ref[0:1, span]
        value = own[face][...] - shared * far[face][...]
        if initial:
            value = rhs_ref[:, span] - shared * rhs_far_ref[:, span] - value
        out_ref[:, span] = value
        for mode in range(MODES):
            totals[mode] += value * modes_ref[mode : mode + 1, span]
        if not initial:
            weights = masks_ref[1:2, span]
            weighted_w = weights * w_ref[:, span]
            totals[MODES] += weighted_w * w_ref[:, span]
            totals[MODES + 1] += weighted_w * value
            totals[MODES + 2] += weighted_w * q_ref[:, span]
            totals[MODES + 3] += weights * d_ref[:, span] * value
    lane = lax.broadcasted_iota(jnp.int32, sums_ref.shape, 1)
    result = jnp.zeros(sums_ref.shape, jnp.float32)
    for index, total in enumerate(totals):
        place = slot_ref[0] * MODES + index if index < MODES else slots * MODES + index - MODES
        result = jnp.where(lane == place, jnp.sum(total, axis=1, keepdims=True), result)
    sums_ref[...] = result


def per_device(
    dual_blocks, rigid_modes, dual_local, coarse_rhs, iface_sizes, neighbours, shared_counts,
    iface_map, owner,
):
    my_slot = lax.axis_index("dev")
    slots = lax.axis_size("dev")
    loads, nmax = dual_local.shape[1:]
    cap = nmax // FACES
    blocks = nmax // LANES
    size = slots * MODES
    width = -(-(size + 4) // LANES) * LANES
    steps = nmax // ROWS
    f32 = jnp.float32
    shape = jax.ShapeDtypeStruct
    vector, face_vec = shape((loads, nmax), f32), shape((loads, cap), f32)
    scalar_shape, sums_shape = shape((loads, LANES), f32), shape((loads, width), f32)

    live = jnp.arange(nmax, dtype=jnp.int32) < iface_sizes[0]
    codes = jnp.where(live, iface_map[0], -1)
    code_table = codes.reshape(blocks, LANES)
    padded = jnp.pad(rigid_modes[0], ((0, loads - MODES), (0, 0)))
    modes, rhs, inverse = pl.pallas_call(
        setup_kernel,
        out_shape=(vector, vector, shape((blocks, LANES), jnp.int32)),
        scratch_shapes=[
            pltpu.VMEM((LANES, nmax), jnp.bfloat16),
            pltpu.VMEM((3 * 32, nmax), jnp.bfloat16),
        ],
        compiler_params=params(),
    )(codes.reshape(1, nmax), jnp.stack([padded, dual_local[0]]))

    def exchange(pieces):
        return [
            lax.ppermute(
                pieces[face ^ 1], "dev",
                [(i, (i - FACE_STEPS[face]) % slots) for i in range(slots)],
            )
            for face in range(FACES)
        ]

    both = jnp.concatenate([modes, rhs], axis=0)
    far_pieces = exchange([both[:, f * cap : (f + 1) * cap] for f in range(FACES)])
    position = jnp.arange(cap, dtype=jnp.int32)
    counted = position[None, :] < shared_counts[0][:, None]
    shared = (counted & (neighbours[0] >= 0)[:, None]).astype(f32).reshape(1, nmax)
    weights = counted.astype(f32).reshape(1, nmax) - 0.5 * shared
    masks = jnp.concatenate([shared, weights, jnp.zeros((6, nmax), f32)], axis=0)
    far_both = jnp.concatenate(far_pieces, axis=1) * shared
    far_modes, far_rhs = far_both[:loads], far_both[loads:]

    own6 = modes[:MODES].reshape(MODES, FACES, cap)
    far6 = far_modes[:MODES].reshape(MODES, FACES, cap)
    diagonal = lax.dot_general(
        modes[:MODES], modes[:MODES], (((1,), (1,)), ((), ())), precision=HIGHEST
    )
    coupling = -jnp.einsum("afp,bfp->fab", own6, far6, precision=HIGHEST)
    ids = jnp.arange(slots, dtype=jnp.int32)
    row = jnp.where((ids == my_slot)[None, :, None], diagonal[:, None, :], 0.0)
    for face in range(FACES):
        target = (my_slot + FACE_STEPS[face]) % slots
        row += jnp.where((ids == target)[None, :, None], coupling[face][:, None, :], 0.0)
    row = row.reshape(MODES, size)
    row = jnp.concatenate(
        [row, jnp.pad(coarse_rhs[0], ((0, 0), (0, width - size - loads)))]
        if width - size >= loads
        else [row, jnp.pad(coarse_rhs[0], ((0, 0), (0, LANES - loads)))],
        axis=1,
    )
    everything = lax.all_gather(row, "dev", axis=0, tiled=True)
    goal = jnp.pad(everything[:, size : size + loads].T, ((0, 0), (0, width - size)))
    matrix = jnp.pad(everything[:, :size], ((0, 0), (0, width - size)))
    inverted = pl.pallas_call(
        invert_kernel,
        out_shape=shape((size, width), f32),
        compiler_params=params(),
    )(matrix)
    groups = [
        lax.dynamic_slice(inverted, (((my_slot + by) % slots) * MODES, 0), (MODES, width))
        for by in (0,) + FACE_STEPS
    ]
    picks = jnp.pad(
        jnp.concatenate(groups, axis=0), ((0, LANES - MODES * (FACES + 1)), (0, 0))
    ).T
    picks = jnp.where((jnp.arange(width) < size)[:, None], picks, 0.0)

    def whole(item):
        return pl.BlockSpec(item.shape, lambda i, rank=len(item.shape): (0,) * rank)

    def with_product(kernel, ins, outs, *static):
        out_shape = tuple(outs) + (face_vec,) * FACES
        return pl.pallas_call(
            functools.partial(kernel, steps, cap, *static),
            grid=(steps,),
            in_specs=[whole(x) for x in ins]
            + [pl.BlockSpec((1, ROWS, nmax), lambda i: (0, i, 0))],
            out_specs=tuple(whole(x) for x in out_shape),
            out_shape=out_shape,
            scratch_shapes=[pltpu.VMEM((loads, nmax), f32)],
            compiler_params=params(steps),
        )(*ins, dual_blocks)

    slot_array = my_slot.reshape(1).astype(jnp.int32)

    def combine(own, extra, initial):
        far = exchange(own)
        ins = (modes, masks, *own, *far, *extra)
        value, sums = pl.pallas_call(
            functools.partial(combine_kernel, cap, slots, initial),
            in_specs=[pl.BlockSpec(memory_space=pltpu.SMEM)]
            + [pl.BlockSpec(memory_space=pltpu.VMEM)] * len(ins),
            out_shape=(vector, sums_shape),
            compiler_params=params(),
        )(slot_array, *ins)
        return value, lax.all_gather(sums, "dev", axis=0)

    mult, *own = with_product(
        start_kernel, (goal, picks, modes, far_modes, code_table, inverse), (vector,)
    )
    residual, gathered = combine(own, (rhs, far_rhs), True)
    w, *own = with_product(
        first_kernel, (gathered, picks, modes, far_modes, residual, code_table, inverse), (vector,)
    )
    d = q = s = jnp.zeros((loads, nmax), f32)
    scalars = jnp.broadcast_to(
        jnp.where(jnp.arange(LANES) == 0, 1.0, 0.0).astype(f32), (loads, LANES)
    )
    for step in range(ITERS):
        applied, gathered = combine(own, (w, d, q), False)
        ins = (gathered, picks, modes, far_modes, mult, w, d, q, s, applied, scalars, code_table)
        if step < ITERS - 1:
            mult, w, d, q, s, scalars, *own = with_product(
                step_kernel, ins + (inverse,), (vector,) * 5 + (scalar_shape,), slots
            )
    return pl.pallas_call(
        functools.partial(last_kernel, cap, slots),
        out_shape=(shape((1, loads, nmax), f32),) * 2,
        scratch_shapes=[pltpu.VMEM((loads, nmax), f32)] * 2,
        compiler_params=params(),
    )(*ins)


def solution(mesh):
    return jax.shard_map(
        per_device,
        mesh=mesh,
        in_specs=(
            P("dev", None, None),
            P("dev", None, None),
            P("dev", None, None),
            P("dev", None, None),
            P("dev"),
            P("dev", None),
            P("dev", None),
            P("dev", None),
            P(),
        ),
        out_specs=(P("dev", None, None), P("dev", None, None)),
        check_vma=False,
    )
```

```python
import functools

import jax
import jax.numpy as jnp
from jax import lax
from jax.experimental import pallas as pl
from jax.experimental.pallas import tpu as pltpu
from jax.sharding import PartitionSpec as P

FACES = 6
MODES = 6
ITERS = 3
LANES = 128
ROWS = 256
FACE_STEPS = (-1, 1, -4, 4, -16, 16)
HIGHEST = lax.Precision.HIGHEST


def params(steps=None):
    if steps is None:
        return pltpu.CompilerParams(vmem_limit_bytes=50 * 2**20)
    return pltpu.CompilerParams(
        dimension_semantics=("arbitrary",), vmem_limit_bytes=50 * 2**20
    )


def gather_lanes(source, index_ref, block):
    index = jnp.broadcast_to(index_ref[pl.ds(block, 1), :], (source.shape[0], LANES))
    low = jnp.bitwise_and(index, LANES - 1)
    high = jnp.right_shift(index, 7)
    picked = jnp.zeros((source.shape[0], LANES), jnp.float32)
    for part in range(source.shape[1] // LANES):
        taken = jnp.take_along_axis(
            source[:, part * LANES : (part + 1) * LANES], low, axis=1, mode="promise_in_bounds"
        )
        picked = jnp.where(high == part, taken, picked)
    return picked


def setup_kernel(codes_ref, values_ref, modes_ref, rhs_ref, inverse_ref, onehot_ref, left_ref):
    codes = codes_ref[...]
    nmax = codes.shape[1]
    blocks = nmax // LANES
    wide = left_ref.shape[0] // 3
    columns = lax.broadcasted_iota(jnp.int32, (1, nmax), 1)
    high = jnp.right_shift(codes, 7)
    low = jnp.where(codes < 0, -1, jnp.bitwise_and(codes, LANES - 1))
    rows = lax.broadcasted_iota(jnp.int32, (LANES, nmax), 0)
    onehot_ref[...] = jnp.where(rows == low, 1.0, 0.0).astype(jnp.bfloat16)
    hit = lax.broadcasted_iota(jnp.int32, (wide, nmax), 0) == high
    upper = jnp.right_shift(columns, 7).astype(jnp.float32)
    lower = jnp.bitwise_and(columns, LANES - 1).astype(jnp.float32)
    left_ref[:wide, :] = jnp.where(hit, upper, 0.0).astype(jnp.bfloat16)
    left_ref[wide : 2 * wide, :] = jnp.where(hit, lower, 0.0).astype(jnp.bfloat16)
    left_ref[2 * wide :, :] = jnp.where(hit, 1.0, 0.0).astype(jnp.bfloat16)
    found = lax.dot_general(
        left_ref[...], onehot_ref[...], (((1,), (1,)), ((), ())),
        preferred_element_type=jnp.float32,
    )
    place = found[:wide] * LANES + found[wide : 2 * wide]
    place = jnp.where(found[2 * wide :] > 0.5, place, float(nmax))
    inverse_ref[...] = (place[:blocks] + 0.5).astype(jnp.int32)

    def body(block, carry):
        start = pl.multiple_of(block * LANES, LANES)
        modes_ref[:, pl.ds(start, LANES)] = gather_lanes(values_ref.at[0], inverse_ref, block)
        rhs_ref[:, pl.ds(start, LANES)] = gather_lanes(values_ref.at[1], inverse_ref, block)
        return carry

    lax.fori_loop(0, blocks, body, 0)


def invert_kernel(matrix_ref, out_ref):
    size, width = out_ref.shape
    out_ref[...] = matrix_ref[...]
    lane = lax.broadcasted_iota(jnp.int32, (1, width), 1)

    def body(step, carry):
        k = 2 * step
        at0, at1 = lane == k, lane == k + 1
        row0 = out_ref[pl.ds(k, 1), :]
        row1 = out_ref[pl.ds(k + 1, 1), :]
        p00 = jnp.sum(jnp.where(at0, row0, 0.0), axis=1, keepdims=True)
        p01 = jnp.sum(jnp.where(at1, row0, 0.0), axis=1, keepdims=True)
        p11 = jnp.sum(jnp.where(at1, row1, 0.0), axis=1, keepdims=True)
        first = 1.0 / p00
        ratio = p01 * first
        i11 = 1.0 / (p11 - p01 * ratio)
        i01 = -ratio * i11
        i00 = first + ratio * ratio * i11
        use0 = i00 * row0 + i01 * row1
        use1 = i01 * row0 + i11 * row1
        whole = out_ref[...]
        col0 = jnp.sum(jnp.where(at0, whole, 0.0), axis=1, keepdims=True)
        col1 = jnp.sum(jnp.where(at1, whole, 0.0), axis=1, keepdims=True)
        fresh = whole - col0 * use0 - col1 * use1
        fresh = jnp.where(at0, col0 * i00 + col1 * i01, fresh)
        fresh = jnp.where(at1, col0 * i01 + col1 * i11, fresh)
        out_ref[...] = fresh
        out_ref[pl.ds(k, 1), :] = jnp.where(at0, -i00, jnp.where(at1, -i01, use0))
        out_ref[pl.ds(k + 1, 1), :] = jnp.where(at0, -i01, jnp.where(at1, -i11, use1))
        return carry

    lax.fori_loop(0, size // 2, body, 0)
    out_ref[...] = -out_ref[...]


def coarse_apply(coarse, picks_ref, modes_ref, far_ref, cap):
    z = lax.dot_general(
        coarse, picks_ref[...], (((1,), (0,)), ((), ())),
        precision=HIGHEST, preferred_element_type=jnp.float32,
    )
    blocks = []
    for face in range(FACES):
        span = slice(face * cap, (face + 1) * cap)
        total = jnp.zeros((coarse.shape[0], cap), jnp.float32)
        for mode in range(MODES):
            total += z[:, mode : mode + 1] * modes_ref[mode : mode + 1, span]
            column = (face + 1) * MODES + mode
            total -= z[:, column : column + 1] * far_ref[mode : mode + 1, span]
        blocks.append(total)
    return blocks


def product_steps(step, steps, vector_ref, map_ref, inverse_ref, dual_ref, sum_ref, outs, cap):
    per_step = dual_ref.shape[1] // LANES
    pieces = [gather_lanes(vector_ref, map_ref, step * per_step + i) for i in range(per_step)]
    vector = jnp.concatenate(pieces, axis=1).astype(jnp.bfloat16)
    part = jnp.dot(vector, dual_ref[0], preferred_element_type=jnp.float32)

    @pl.when(step == 0)
    def _():
        sum_ref[...] = part

    @pl.when(step > 0)
    def _():
        sum_ref[...] += part

    @pl.when(step == steps - 1)
    def _():
        def body(block, carry):
            start = pl.multiple_of(block * LANES, LANES)
            for face in range(FACES):
                outs[face][:, pl.ds(start, LANES)] = gather_lanes(
                    sum_ref, inverse_ref, face * (cap // LANES) + block
                )
            return carry

        lax.fori_loop(0, cap // LANES, body, 0)


def start_kernel(
    steps, cap, coarse_ref, picks_ref, modes_ref, far_ref, map_ref, inverse_ref, dual_ref,
    mult_ref, *rest,
):
    outs, sum_ref = rest[:FACES], rest[FACES]
    step = pl.program_id(0)

    @pl.when(step == 0)
    def _():
        parts = coarse_apply(coarse_ref[...], picks_ref, modes_ref, far_ref, cap)
        for face, part in enumerate(parts):
            mult_ref[:, face * cap : (face + 1) * cap] = part

    product_steps(step, steps, mult_ref, map_ref, inverse_ref, dual_ref, sum_ref, outs, cap)


def first_kernel(
    steps, cap, gathered_ref, picks_ref, modes_ref, far_ref, residual_ref, map_ref, inverse_ref,
    dual_ref, w_ref, *rest,
):
    outs, sum_ref = rest[:FACES], rest[FACES]
    step = pl.program_id(0)

    @pl.when(step == 0)
    def _():
        coarse = jnp.sum(gathered_ref[...], axis=0)
        parts = coarse_apply(coarse, picks_ref, modes_ref, far_ref, cap)
        for face, part in enumerate(parts):
            span = slice(face * cap, (face + 1) * cap)
            w_ref[:, span] = residual_ref[:, span] - part

    product_steps(step, steps, w_ref, map_ref, inverse_ref, dual_ref, sum_ref, outs, cap)


def advance(
    cap, slots, gathered_ref, picks_ref, modes_ref, far_ref, state, applied_ref, scalars_ref, outs
):
    mult_ref, w_ref, d_ref, q_ref, s_ref = state
    mult_out, w_out, d_out, q_out, s_out, scalars_out = outs
    coarse = jnp.sum(gathered_ref[...], axis=0)
    base = slots * MODES
    rho, wa, wq, da = (coarse[:, base + i : base + i + 1] for i in range(4))
    rho_old, dq_old = scalars_ref[:, 0:1], scalars_ref[:, 1:2]
    beta = rho / rho_old
    dq = wa + beta * (wq + da) + beta * beta * dq_old
    alpha = rho / dq
    parts = coarse_apply(coarse, picks_ref, modes_ref, far_ref, cap)
    for face, part in enumerate(parts):
        span = slice(face * cap, (face + 1) * cap)
        applied = applied_ref[:, span]
        d = w_ref[:, span] + beta * d_ref[:, span]
        s = applied - part + beta * s_ref[:, span]
        mult_out[:, span] = mult_ref[:, span] + alpha * d
        w_out[:, span] = w_ref[:, span] - alpha * s
        if d_out is not None:
            d_out[:, span] = d
            s_out[:, span] = s
            q_out[:, span] = applied + beta * q_ref[:, span]
    if scalars_out is not None:
        lane = lax.broadcasted_iota(jnp.int32, scalars_out.shape, 1)
        scalars_out[...] = jnp.where(lane == 0, rho, jnp.where(lane == 1, dq, 0.0))


def step_kernel(
    steps, cap, slots, gathered_ref, picks_ref, modes_ref, far_ref, m_ref, w_ref, d_ref, q_ref,
    s_ref, applied_ref, scalars_ref, map_ref, inverse_ref, dual_ref,
    m_out, w_out, d_out, q_out, s_out, scalars_out, *rest,
):
    outs, sum_ref = rest[:FACES], rest[FACES]
    step = pl.program_id(0)

    @pl.when(step == 0)
    def _():
        advance(
            cap, slots, gathered_ref, picks_ref, modes_ref, far_ref,
            (m_ref, w_ref, d_ref, q_ref, s_ref), applied_ref, scalars_ref,
            (m_out, w_out, d_out, q_out, s_out, scalars_out),
        )

    product_steps(step, steps, w_out, map_ref, inverse_ref, dual_ref, sum_ref, outs, cap)


def last_kernel(
    cap, slots, gathered_ref, picks_ref, modes_ref, far_ref, m_ref, w_ref, d_ref, q_ref, s_ref,
    applied_ref, scalars_ref, map_ref, m_out, w_out, m_tmp, w_tmp,
):
    advance(
        cap, slots, gathered_ref, picks_ref, modes_ref, far_ref,
        (m_ref, w_ref, d_ref, q_ref, s_ref), applied_ref, scalars_ref,
        (m_tmp, w_tmp, None, None, None, None),
    )

    def body(block, carry):
        start = pl.multiple_of(block * LANES, LANES)
        m_out[0, :, pl.ds(start, LANES)] = gather_lanes(m_tmp, map_ref, block)
        w_out[0, :, pl.ds(start, LANES)] = gather_lanes(w_tmp, map_ref, block)
        return carry

    lax.fori_loop(0, m_tmp.shape[1] // LANES, body, 0)


def greet(partners):
    barrier = pltpu.get_barrier_semaphore()
    for partner in partners:
        pl.semaphore_signal(
            barrier, inc=1, device_id=(partner,), device_id_type=pl.DeviceIdType.MESH
        )
    pl.semaphore_wait(barrier, len(partners))


def face_copies(pieces, land_ref, send_sem, recv_sem, slots):
    me = lax.axis_index("dev")
    targets = [lax.rem(me + by + slots, slots) for by in FACE_STEPS]
    greet(targets)
    copies = [
        pltpu.make_async_remote_copy(
            src_ref=pieces[face],
            dst_ref=land_ref.at[face ^ 1],
            send_sem=send_sem.at[face],
            recv_sem=recv_sem.at[face ^ 1],
            device_id=(targets[face],),
            device_id_type=pl.DeviceIdType.MESH,
        )
        for face in range(FACES)
    ]
    for copy in copies:
        copy.start()
    return copies


def exchange_kernel(slots, *refs):
    pieces, out_ref, (land_ref, send_sem, recv_sem) = refs[:FACES], refs[FACES], refs[FACES + 1 :]
    cap = land_ref.shape[2]
    for copy in face_copies(pieces, land_ref, send_sem, recv_sem, slots):
        copy.wait()
    for face in range(FACES):
        out_ref[:, face * cap : (face + 1) * cap] = land_ref[face]


def everyone_kernel(slots, total, own_ref, out_ref, land_ref, send_sem, recv_sem):
    me = lax.axis_index("dev")
    barrier = pltpu.get_barrier_semaphore()

    def signal(by, carry):
        pl.semaphore_signal(
            barrier, inc=1, device_id=(lax.rem(me + by, slots),),
            device_id_type=pl.DeviceIdType.MESH,
        )
        return carry

    lax.fori_loop(1, slots, signal, 0)
    pl.semaphore_wait(barrier, slots - 1)

    def copy(by):
        return pltpu.make_async_remote_copy(
            src_ref=own_ref,
            dst_ref=land_ref.at[me],
            send_sem=send_sem.at[by],
            recv_sem=recv_sem.at[by],
            device_id=(lax.rem(me + by, slots),),
            device_id_type=pl.DeviceIdType.MESH,
        )

    def start(by, carry):
        copy(by).start()
        return carry

    def finish(by, carry):
        copy(by).wait()
        return carry

    lax.fori_loop(1, slots, start, 0)
    land_ref[me] = own_ref[...]
    lax.fori_loop(1, slots, finish, 0)
    if total:
        out_ref[0] = jnp.sum(land_ref[...], axis=0)
    else:
        out_ref[...] = land_ref[...]


def combine_kernel(cap, slots, initial, slot_ref, modes_ref, masks_ref, *rest):
    own, rest = rest[:FACES], rest[FACES:]
    rest, (far, send_sem, recv_sem) = rest[:-3], rest[-3:]
    if initial:
        rhs_ref, rhs_far_ref, out_ref, sums_ref = rest
    else:
        w_ref, d_ref, q_ref, out_ref, sums_ref = rest
    loads = own[0].shape[0]
    counts = MODES if initial else MODES + 4
    totals = [jnp.zeros((loads, cap), jnp.float32) for _ in range(counts)]
    for copy in face_copies(own, far, send_sem, recv_sem, slots):
        copy.wait()
    for face in range(FACES):
        span = slice(face * cap, (face + 1) * cap)
        shared = masks_ref[0:1, span]
        value = own[face][...] - shared * far[face]
        if initial:
            value = rhs_ref[:, span] - shared * rhs_far_ref[:, span] - value
        out_ref[:, span] = value
        for mode in range(MODES):
            totals[mode] += value * modes_ref[mode : mode + 1, span]
        if not initial:
            weights = masks_ref[1:2, span]
            weighted_w = weights * w_ref[:, span]
            totals[MODES] += weighted_w * w_ref[:, span]
            totals[MODES + 1] += weighted_w * value
            totals[MODES + 2] += weighted_w * q_ref[:, span]
            totals[MODES + 3] += weights * d_ref[:, span] * value
    lane = lax.broadcasted_iota(jnp.int32, sums_ref.shape, 1)
    result = jnp.zeros(sums_ref.shape, jnp.float32)
    for index, total in enumerate(totals):
        place = slot_ref[0] * MODES + index if index < MODES else slots * MODES + index - MODES
        result = jnp.where(lane == place, jnp.sum(total, axis=1, keepdims=True), result)
    sums_ref[...] = result


def per_device(
    dual_blocks, rigid_modes, dual_local, coarse_rhs, iface_sizes, neighbours, shared_counts,
    iface_map, owner,
):
    my_slot = lax.axis_index("dev")
    slots = lax.axis_size("dev")
    loads, nmax = dual_local.shape[1:]
    cap = nmax // FACES
    blocks = nmax // LANES
    size = slots * MODES
    width = -(-(size + 4) // LANES) * LANES
    steps = nmax // ROWS
    f32 = jnp.float32
    shape = jax.ShapeDtypeStruct
    vector, face_vec = shape((loads, nmax), f32), shape((loads, cap), f32)
    scalar_shape, sums_shape = shape((loads, LANES), f32), shape((loads, width), f32)

    live = jnp.arange(nmax, dtype=jnp.int32) < iface_sizes[0]
    codes = jnp.where(live, iface_map[0], -1)
    code_table = codes.reshape(blocks, LANES)
    padded = jnp.pad(rigid_modes[0], ((0, loads - MODES), (0, 0)))
    modes, rhs, inverse = pl.pallas_call(
        setup_kernel,
        out_shape=(vector, vector, shape((blocks, LANES), jnp.int32)),
        scratch_shapes=[
            pltpu.VMEM((LANES, nmax), jnp.bfloat16),
            pltpu.VMEM((3 * 32, nmax), jnp.bfloat16),
        ],
        compiler_params=params(),
    )(codes.reshape(1, nmax), jnp.stack([padded, dual_local[0]]))

    def linked(name):
        return pltpu.CompilerParams(
            collective_id=name, has_side_effects=True, vmem_limit_bytes=50 * 2**20
        )

    def face_scratch(rows):
        return [
            pltpu.VMEM((FACES, rows, cap), f32),
            pltpu.SemaphoreType.DMA((FACES,)),
            pltpu.SemaphoreType.DMA((FACES,)),
        ]

    def everyone(block, total):
        return pl.pallas_call(
            functools.partial(everyone_kernel, slots, total),
            out_shape=shape((1 if total else slots,) + block.shape, f32),
            scratch_shapes=[
                pltpu.VMEM((slots,) + block.shape, f32),
                pltpu.SemaphoreType.DMA((slots,)),
                pltpu.SemaphoreType.DMA((slots,)),
            ],
            compiler_params=linked(0 if total else 4),
        )(block)

    both = jnp.concatenate([modes, rhs], axis=0)
    far_both = pl.pallas_call(
        functools.partial(exchange_kernel, slots),
        out_shape=shape((2 * loads, nmax), f32),
        scratch_shapes=face_scratch(2 * loads),
        compiler_params=linked(3),
    )(*[both[:, f * cap : (f + 1) * cap] for f in range(FACES)])
    position = jnp.arange(cap, dtype=jnp.int32)
    counted = position[None, :] < shared_counts[0][:, None]
    shared = (counted & (neighbours[0] >= 0)[:, None]).astype(f32).reshape(1, nmax)
    weights = counted.astype(f32).reshape(1, nmax) - 0.5 * shared
    masks = jnp.concatenate([shared, weights, jnp.zeros((6, nmax), f32)], axis=0)
    far_both = far_both * shared
    far_modes, far_rhs = far_both[:loads], far_both[loads:]

    own6 = modes[:MODES].reshape(MODES, FACES, cap)
    far6 = far_modes[:MODES].reshape(MODES, FACES, cap)
    diagonal = lax.dot_general(
        modes[:MODES], modes[:MODES], (((1,), (1,)), ((), ())), precision=HIGHEST
    )
    coupling = -jnp.einsum("afp,bfp->fab", own6, far6, precision=HIGHEST)
    ids = jnp.arange(slots, dtype=jnp.int32)
    row = jnp.where((ids == my_slot)[None, :, None], diagonal[:, None, :], 0.0)
    for face in range(FACES):
        target = (my_slot + FACE_STEPS[face]) % slots
        row += jnp.where((ids == target)[None, :, None], coupling[face][:, None, :], 0.0)
    row = row.reshape(MODES, size)
    row = jnp.concatenate(
        [row, jnp.pad(coarse_rhs[0], ((0, 0), (0, width - size - loads)))]
        if width - size >= loads
        else [row, jnp.pad(coarse_rhs[0], ((0, 0), (0, LANES - loads)))],
        axis=1,
    )
    everything = everyone(jnp.pad(row, ((0, loads - MODES), (0, 0))), False)
    everything = everything[:, :MODES].reshape(size, row.shape[1])
    goal = jnp.pad(everything[:, size : size + loads].T, ((0, 0), (0, width - size)))
    matrix = jnp.pad(everything[:, :size], ((0, 0), (0, width - size)))
    inverted = pl.pallas_call(
        invert_kernel,
        out_shape=shape((size, width), f32),
        compiler_params=params(),
    )(matrix)
    groups = [
        lax.dynamic_slice(inverted, (((my_slot + by) % slots) * MODES, 0), (MODES, width))
        for by in (0,) + FACE_STEPS
    ]
    picks = jnp.pad(
        jnp.concatenate(groups, axis=0), ((0, LANES - MODES * (FACES + 1)), (0, 0))
    ).T
    picks = jnp.where((jnp.arange(width) < size)[:, None], picks, 0.0)

    def whole(item):
        return pl.BlockSpec(item.shape, lambda i, rank=len(item.shape): (0,) * rank)

    def with_product(kernel, ins, outs, *static):
        out_shape = tuple(outs) + (face_vec,) * FACES
        return pl.pallas_call(
            functools.partial(kernel, steps, cap, *static),
            grid=(steps,),
            in_specs=[whole(x) for x in ins]
            + [pl.BlockSpec((1, ROWS, nmax), lambda i: (0, i, 0))],
            out_specs=tuple(whole(x) for x in out_shape),
            out_shape=out_shape,
            scratch_shapes=[pltpu.VMEM((loads, nmax), f32)],
            compiler_params=params(steps),
        )(*ins, dual_blocks)

    slot_array = my_slot.reshape(1).astype(jnp.int32)

    def combine(own, extra, initial):
        ins = (modes, masks, *own, *extra)
        value, sums = pl.pallas_call(
            functools.partial(combine_kernel, cap, slots, initial),
            in_specs=[pl.BlockSpec(memory_space=pltpu.SMEM)]
            + [pl.BlockSpec(memory_space=pltpu.VMEM)] * len(ins),
            out_shape=(vector, sums_shape),
            scratch_shapes=face_scratch(loads),
            compiler_params=linked(1 if initial else 2),
        )(slot_array, *ins)
        return value, everyone(sums, True)

    mult, *own = with_product(
        start_kernel, (goal, picks, modes, far_modes, code_table, inverse), (vector,)
    )
    residual, gathered = combine(own, (rhs, far_rhs), True)
    w, *own = with_product(
        first_kernel, (gathered, picks, modes, far_modes, residual, code_table, inverse), (vector,)
    )
    d = q = s = jnp.zeros((loads, nmax), f32)
    scalars = jnp.broadcast_to(
        jnp.where(jnp.arange(LANES) == 0, 1.0, 0.0).astype(f32), (loads, LANES)
    )
    for step in range(ITERS):
        applied, gathered = combine(own, (w, d, q), False)
        ins = (gathered, picks, modes, far_modes, mult, w, d, q, s, applied, scalars, code_table)
        if step < ITERS - 1:
            mult, w, d, q, s, scalars, *own = with_product(
                step_kernel, ins + (inverse,), (vector,) * 5 + (scalar_shape,), slots
            )
    return pl.pallas_call(
        functools.partial(last_kernel, cap, slots),
        out_shape=(shape((1, loads, nmax), f32),) * 2,
        scratch_shapes=[pltpu.VMEM((loads, nmax), f32)] * 2,
        compiler_params=params(),
    )(*ins)


def solution(mesh):
    return jax.shard_map(
        per_device,
        mesh=mesh,
        in_specs=(
            P("dev", None, None),
            P("dev", None, None),
            P("dev", None, None),
            P("dev", None, None),
            P("dev"),
            P("dev", None),
            P("dev", None),
            P("dev", None),
            P(),
        ),
        out_specs=(P("dev", None, None), P("dev", None, None)),
        check_vma=False,
    )
```
